128 devices in a mesh: tp: 4 (over y_hi, core), grp: 32 (over z, x, y_lo).
Axes of the slice: x: 4, y: 4 (y_hi: 2, y_lo: 2; y = y_hi * 2 + y_lo), z: 4, core: 2. Of those that a mesh axis runs over, the one named last changes fastest.
Arguments:
- teacher_state: bfloat16 [8192, 5280], P('grp'), may hold values from -6 to 6
- injection: bfloat16 [8192, 5280], P('grp'), may hold values from -6 to 6
- teacher_up: bfloat16 [5280, 8960], P(None, 'tp'), may hold values from -0.078125 to 0.078125
- teacher_down: bfloat16 [8960, 5280], P('tp', 'grp'), may hold values from -0.0625 to 0.0625
- student_up: bfloat16 [5280, 256], P('grp', 'tp'), may hold values from -0.078125 to 0.078125
- student_down: bfloat16 [256, 5280], P('tp', 'grp'), may hold values from -0.375 to 0.375
- teacher_step: int32 [8], replicated, may hold values from 0 to 1
- student_depth: int32 [8], replicated, may hold values from 1 to 2
Outputs:
- grad_up: float32 [5280, 256], P('grp', 'tp')
- grad_down: float32 [256, 5280], P('tp', 'grp')
The draws below stay inside these ranges and needn't reach their ends.
All inputs are finite; a program needn't handle non-finite values.
Results may differ from the reference program's by a relative error of at most 0.02.
Values may be sent and summed in bfloat16 or wider, within the bound.
A program may use at most 192 MiB of HBM per device.

```python
import jax
import jax.numpy as jnp
from jax import lax

D = 5280
SH = 256
TOK_G = 256
LENGTH = 1024
T_ITERS = 1
S_ITERS = 2
H_T = 8960
TOKENS = 8192
SEQS = 8
N_TP = 4
N_GRP = 32


def with_ends(drawn, key, smallest, largest):
    dims = drawn.shape
    place = [jax.random.randint(jax.random.fold_in(key, axis), (), 0, dims[axis]) for axis in range(len(dims))]
    drawn = drawn.at[tuple(place)].set(smallest)
    longest = dims.index(max(dims))
    place[longest] = (place[longest] + 1) % dims[longest]
    return drawn.at[tuple(place)].set(largest)


def raised(values, rng, source, target, parts, factor):
    def block_of(axis_at):
        return (jnp.arange(values.shape[axis_at]) // (values.shape[axis_at] // parts)).reshape((-1,) + (1,) * (values.ndim - 1 - axis_at))

    near = jax.random.permutation(rng, parts)[block_of(target)]
    other_side = (block_of(target) + parts // 2) % parts
    return jnp.where((block_of(source) == near) | (block_of(source) == other_side), factor * values, values)


def block_scale(stream_key, shape, shards, least, high):
    def one(position, blocks):
        heights = jax.random.uniform(jax.random.fold_in(jax.random.fold_in(stream_key, 6), position), (blocks,), jnp.float32, least / len(shards), high / len(shards))
        return jnp.repeat(jnp.exp(heights), shape[position] // blocks).reshape((-1,) + (1,) * (len(shape) - position - 1))

    gain = one(*shards[0])
    for cut in shards[1:]:
        gain = gain * one(*cut)
    return gain


def gaussian(own_key, shape, deviation, reach, cuts=(), kind=jnp.bfloat16):
    array = jax.random.normal(own_key, shape, jnp.float32) * deviation
    if len(cuts) > 0:
        array = block_scale(own_key, shape, cuts, -0.22, 0.18) * array
    return jnp.clip(array, min=-reach, max=reach).astype(kind)


def noise_with(rng, extent, deviation, limit, split, heavy, held_as=jnp.bfloat16):
    values = deviation * jax.random.normal(rng, extent, jnp.float32)
    if split:
        values = values * block_scale(rng, extent, split, -0.22, 0.18)
    return jnp.clip(raised(values, jax.random.fold_in(rng, 3), *heavy), -limit, limit).astype(held_as)


def setup_inputs(seed: int = 0) -> dict:
    seeds = jax.random.split(jax.random.key(seed), 9)
    teacher_state = gaussian(seeds[0], (TOKENS, D), 1.0, 6.0, ((0, 32),))
    injection = noise_with(seeds[1], (TOKENS, D), 1.0, 6.0, ((0, 32),), (0, 1, 32, 2.75))
    teacher_up = gaussian(seeds[2], (D, H_T), D ** -0.5, 0.078125, ((1, 4),))
    teacher_down = gaussian(seeds[3], (H_T, D), H_T ** -0.5, 0.0625, ((0, 4), (1, 32)))
    student_up = gaussian(seeds[4], (D, SH), D ** -0.5, 0.078125, ((0, 32), (1, 4)))
    student_down = gaussian(seeds[5], (SH, D), SH ** -0.5, 0.375, ((0, 4), (1, 32)))
    teacher_step = with_ends(jax.random.randint(seeds[6], (SEQS,), 0, T_ITERS + 1), jax.random.fold_in(seeds[6], 1), 0, T_ITERS).astype(jnp.int32)
    student_depth = with_ends(jax.random.randint(seeds[7], (SEQS,), 1, S_ITERS + 1), jax.random.fold_in(seeds[7], 1), 1, S_ITERS).astype(jnp.int32)
    return dict(teacher_state=teacher_state, injection=injection, teacher_up=teacher_up, teacher_down=teacher_down, student_up=student_up, student_down=student_down, teacher_step=teacher_step, student_depth=student_depth)


epsilon = 1e-06
loss_scale = 64.0

def normalize(summed):
    return lax.rsqrt(lax.optimization_barrier(jnp.mean(summed * summed, axis=-1, keepdims=True)) + epsilon)

def silu_slope(logits):
    sigmoid = jax.nn.sigmoid(logits)
    return sigmoid * (1.0 + logits * (1.0 - sigmoid))

def teacher_delta(normed, teacher_up, teacher_down):
    width = teacher_up.shape[1] // N_TP
    totals = jnp.zeros((normed.shape[0], teacher_down.shape[1]), jnp.float32)
    for member in range(N_TP):
        hidden = jax.nn.silu(jnp.dot(normed, teacher_up[:, member * width:(member + 1) * width], preferred_element_type=jnp.float32)).astype(jnp.bfloat16)
        partial_sum = jnp.dot(hidden, teacher_down[member * width:(member + 1) * width], preferred_element_type=jnp.float32).astype(jnp.bfloat16)
        partial_sum = lax.optimization_barrier(partial_sum)
        totals = totals + partial_sum.astype(jnp.float32)
    return totals

def teacher_block(state, injection, teacher_up, teacher_down):
    latents = []
    current = state
    for iteration in range(T_ITERS):
        summed = current.astype(jnp.float32) + injection.astype(jnp.float32)
        normed = (summed * normalize(summed)).astype(jnp.bfloat16)
        current = (current.astype(jnp.float32) + teacher_delta(normed, teacher_up, teacher_down)).astype(jnp.bfloat16)
        latents.append(current)
    return tuple(latents)

def student_grads(start, injection, latents, pick_teacher, pick_depth, student_up, student_down, row_count):
    previous = start
    records = []
    outputs = []
    for iteration in range(S_ITERS):
        summed = previous.astype(jnp.float32) + injection.astype(jnp.float32)
        factor = normalize(summed)
        normed = (summed * factor).astype(jnp.bfloat16)
        logits = jnp.dot(normed, student_up, preferred_element_type=jnp.float32)
        hidden = jax.nn.silu(logits).astype(jnp.bfloat16)
        previous = (previous.astype(jnp.float32) + jnp.dot(hidden, student_down, preferred_element_type=jnp.float32)).astype(jnp.bfloat16)
        records.append((summed, factor, normed, logits, hidden))
        outputs.append(previous)
    target = start.astype(jnp.float32)
    for iteration in range(len(latents)):
        target = jnp.where(pick_teacher[:, None] == iteration + 1, latents[iteration].astype(jnp.float32), target)
    result = jnp.zeros(start.shape, jnp.float32)
    for iteration in range(S_ITERS):
        result = jnp.where(pick_depth[:, None] == iteration + 1, outputs[iteration].astype(jnp.float32), result)
    slope = loss_scale * 2.0 / row_count * (result - target)
    grad_up = jnp.zeros(student_up.shape, jnp.float32)
    grad_down = jnp.zeros(student_down.shape, jnp.float32)
    carried = jnp.zeros(start.shape, jnp.float32)
    for iteration in reversed(range(S_ITERS)):
        summed, factor, normed, logits, hidden = records[iteration]
        cotangent = carried + jnp.where(pick_depth[:, None] == iteration + 1, slope, 0.0)
        rounded = cotangent.astype(jnp.bfloat16)
        grad_down = grad_down + jnp.dot(hidden.T, rounded, preferred_element_type=jnp.float32)
        upstream = jnp.dot(rounded, student_down.T, preferred_element_type=jnp.float32)
        local_grad = (upstream * silu_slope(logits)).astype(jnp.bfloat16)
        grad_up = grad_up + jnp.dot(normed.T, local_grad, preferred_element_type=jnp.float32)
        if iteration > 0:
            back_flow = jnp.dot(local_grad, student_up.T, preferred_element_type=jnp.float32)
            carried = cotangent + factor * back_flow - summed * factor ** 3 * lax.optimization_barrier(jnp.mean(summed * back_flow, axis=-1, keepdims=True))
    return (grad_up, grad_down)

def reference(teacher_state, injection, teacher_up, teacher_down, student_up, student_down, teacher_step, student_depth):
    blocks_state = teacher_state.reshape(N_GRP, TOK_G, D)
    blocks_inject = injection.reshape(N_GRP, TOK_G, D)

    def run_block(paired):
        return teacher_block(paired[0], paired[1], teacher_up, teacher_down)
    stacked = lax.map(run_block, (blocks_state, blocks_inject))
    latents = [member_latent.reshape(TOKENS, D) for member_latent in stacked]
    sequence = jnp.arange(TOKENS, dtype=jnp.int32) // LENGTH
    pick_teacher = teacher_step[sequence]
    pick_depth = student_depth[sequence]
    grad_up, grad_down = student_grads(teacher_state, injection, latents, pick_teacher, pick_depth, student_up, student_down, TOKENS)
    return (grad_up, grad_down)
```

```python
import jax
import jax.numpy as jnp
from jax import lax
from jax.sharding import PartitionSpec as P

LENGTH = 1024
epsilon = 1e-06
loss_scale = 64.0
F32 = jnp.float32
BF16 = jnp.bfloat16


def dot(a, b, dims=((1,), (0,))):
    return lax.dot_general(a, b, (dims, ((), ())), preferred_element_type=F32)


def spread(block, axis):
    size = lax.axis_size(axis)
    tiles = jnp.broadcast_to(block[None], (size, *block.shape))
    return lax.all_to_all(tiles, axis, split_axis=0, concat_axis=0, tiled=True)


def exchange(tiles, axis):
    return lax.all_to_all(tiles, axis, split_axis=0, concat_axis=0, tiled=True)


def total_over(value, axis):
    size = lax.axis_size(axis)
    tiles = value.astype(BF16).reshape(size, value.shape[0] // size, value.shape[1])
    mine = exchange(tiles, axis).astype(F32).sum(axis=0).astype(BF16)
    return spread(mine, axis).reshape(value.shape)


def silu_slope(logits):
    sigmoid = jax.nn.sigmoid(logits)
    return sigmoid * (1.0 + logits * (1.0 - sigmoid))


def body(
    teacher_state,
    injection,
    teacher_up,
    teacher_down,
    student_up,
    student_down,
    teacher_step,
    student_depth,
):
    n_tp, n_grp = lax.axis_size("tp"), lax.axis_size("grp")
    tokens, width = teacher_state.shape
    cols, own = student_up.shape
    units = own * n_tp
    hidden = teacher_down.shape[0]
    scale = loss_scale * 2.0 / (tokens * n_grp)

    pair = jnp.concatenate([student_up.T, student_down], axis=0)
    pairs = spread(pair, "tp")
    up_cols = pairs[:, :own].reshape(units, cols)
    down_cols = pairs[:, own:].reshape(units, cols)
    pair_all = spread(pair, "grp")
    pair_all = jnp.moveaxis(pair_all, 0, 1).reshape(2 * own, width)

    right = jnp.concatenate([teacher_down.T, down_cols.T, up_cols.T], axis=1)
    small = total_over(dot(down_cols, right), "grp")
    teach = small[:, :hidden]
    gram = small[:, hidden : hidden + units]
    cross = small[:, hidden + units :]

    summed = teacher_state.T.astype(F32) + injection.T.astype(F32)
    square = jnp.sum(summed * summed, axis=0, keepdims=True)
    mean1 = square / width + epsilon
    rho1 = lax.rsqrt(mean1)
    norm1 = jnp.sqrt(mean1)
    normed = (summed * rho1).astype(BF16)

    mine = dot(pair_all, normed)
    both = spread(mine, "tp")
    logits1 = both[:, :own].reshape(units, tokens)
    along = both[:, own:].reshape(units, tokens) * norm1
    upward = logits1 * norm1

    teacher_hidden = jax.nn.silu(dot(teacher_up.T, normed)).astype(BF16)
    term = exchange(jnp.broadcast_to(dot(teach, teacher_hidden)[None], (n_tp, units, tokens)), "tp").sum(axis=0)

    first = lax.axis_index("grp") * tokens
    sequence = (first + jnp.arange(tokens, dtype=jnp.int32)) // LENGTH
    matches = sequence[None, :] == jnp.arange(teacher_step.shape[0], dtype=jnp.int32)[:, None]
    taught = jnp.sum(jnp.where(matches, teacher_step[:, None], 0), axis=0, keepdims=True) == 1
    deep = jnp.sum(jnp.where(matches, student_depth[:, None], 0), axis=0, keepdims=True) == 2

    hidden1 = jax.nn.silu(logits1).astype(BF16)
    gram1 = dot(gram, hidden1)
    hidden1_f = hidden1.astype(F32)
    moved = along + gram1
    square2 = square + jnp.sum(hidden1_f * (along + moved), axis=0, keepdims=True)
    rho2 = lax.rsqrt(jnp.maximum(square2, 0.0) / width + epsilon)
    upward2 = upward + dot(cross, hidden1, ((0,), (0,)))
    logits2 = upward2 * rho2
    hidden2 = jnp.where(deep, jax.nn.silu(logits2), 0.0).astype(BF16)
    total = (hidden1_f + hidden2.astype(F32)).astype(BF16)
    taught_total = jnp.where(taught, total, jnp.zeros_like(total))

    slope = scale * (gram1 + dot(gram, hidden2) - jnp.where(taught, term, 0.0))
    q2 = jnp.where(deep, slope * silu_slope(logits2), 0.0)
    mu = jnp.sum(upward2 * q2, axis=0, keepdims=True) / width
    rq2 = (rho2 * q2).astype(BF16)
    ratio = rho2 * rho2 * rho2 * mu
    slope1 = slope + dot(cross, rq2) - ratio * moved
    q1 = slope1 * silu_slope(logits1)

    start = lax.axis_index("tp") * own

    def mine_of(value):
        return lax.dynamic_slice_in_dim(value, start, own, 0)

    rq2_f = rq2.astype(F32)
    left = jnp.concatenate(
        [mine_of(q1 + rq2_f * norm1), mine_of(-hidden1_f * (ratio * norm1))], axis=0
    ).astype(BF16)
    partial = dot(left, normed, ((1,), (1,))).astype(BF16)
    partial = jnp.moveaxis(partial.reshape(2 * own, n_grp, cols), 1, 0)
    direct = exchange(partial, "grp").astype(F32).sum(axis=0)

    weighted = (hidden1_f * ratio).astype(BF16)
    nt = ((1,), (1,))
    c1 = scale * dot(mine_of(total), total, nt) - dot(mine_of(weighted), hidden1, nt)
    c2 = dot(mine_of(hidden1), rq2, nt)
    c3 = dot(mine_of(rq2), hidden1, nt)
    outer = -scale * dot(taught_total, teacher_hidden, nt)
    folded = jnp.concatenate([c1, c2, c3], axis=0).reshape(units, 3 * own)
    summed_all = total_over(jnp.concatenate([outer, folded], axis=1), "grp")
    folded = summed_all[:, hidden:].reshape(3 * own, units)
    through = dot(summed_all[:, :hidden], teacher_down)
    through = exchange(through.reshape(n_tp, own, cols), "tp").sum(axis=0)
    grad_down = direct[own:] + dot(folded[:own], down_cols) + dot(folded[own : 2 * own], up_cols) + through
    grad_up = direct[:own] + dot(folded[2 * own :], down_cols)
    return (grad_up.T, grad_down)


def solution(mesh):
    in_specs = (
        P("grp", None),
        P("grp", None),
        P(None, "tp"),
        P("tp", "grp"),
        P("grp", "tp"),
        P("tp", "grp"),
        P(),
        P(),
    )
    out_specs = (P("grp", "tp"), P("tp", "grp"))
    return jax.shard_map(body, mesh=mesh, in_specs=in_specs, out_specs=out_specs, check_vma=False)
```

```python
import functools

import jax
import jax.numpy as jnp
from jax import lax
from jax.experimental import pallas as pl
from jax.experimental.pallas import tpu as pltpu
from jax.sharding import PartitionSpec as P

LENGTH = 1024
epsilon = 1e-06
loss_scale = 64.0
F32 = jnp.float32
BF16 = jnp.bfloat16
MESH = pl.DeviceIdType.MESH
NN = ((1,), (0,))
NT = ((1,), (1,))
TN = ((0,), (0,))
ROWS = 320
TILE = 128


def dot(a, b, dims=NN):
    return lax.dot_general(a, b, (dims, ((), ())), preferred_element_type=F32)


def silu_slope(logits):
    sigmoid = jax.nn.sigmoid(logits)
    return sigmoid * (1.0 + logits * (1.0 - sigmoid))


def ceil_to(value, multiple):
    return -(-value // multiple) * multiple


def kernel(
    n_tp,
    n_grp,
    sizes,
    state_hbm,
    inject_hbm,
    up_hbm,
    down_hbm,
    tall_ref,
    pair_ref,
    flag_ref,
    direct_ref,
    rest_ref,
    state_v,
    inject_v,
    up_v,
    down_v,
    summed_v,
    normed_v,
    blocks_v,
    hidden_v,
    pairs_v,
    tall_v,
    m_send,
    m_recv,
    m_full,
    g_send,
    g_recv,
    g_full,
    c_send,
    c_recv,
    c_full,
    f_send,
    f_recv,
    z_all,
    small_all,
    term_all,
    term_own,
    out_send,
    out_recv,
    keep,
    load_sem,
    up_sem,
    send_sem,
    recv_sem,
):
    tokens, width, cols, own, hidden, wide, scale = sizes
    units = own * n_tp
    tall = tall_ref.shape[0]
    me_g = lax.axis_index("grp")
    me_t = lax.axis_index("tp")

    def over_grp(slot, source, target):
        def step(k, carry):
            peer = lax.rem(me_g + k, n_grp)
            pltpu.make_async_remote_copy(
                src_ref=source(peer),
                dst_ref=target(k),
                send_sem=send_sem.at[slot],
                recv_sem=recv_sem.at[slot],
                device_id={"grp": peer},
                device_id_type=MESH,
            ).start()
            return carry

        lax.fori_loop(1, n_grp, step, 0)

    def over_tp(slot, source, target):
        for k in range(1, n_tp):
            peer = lax.rem(me_t + k, n_tp)
            pltpu.make_async_remote_copy(
                src_ref=source(peer),
                dst_ref=target(k),
                send_sem=send_sem.at[slot],
                recv_sem=recv_sem.at[slot],
                device_id={"tp": peer},
                device_id_type=MESH,
            ).start()

    def arrived(slot, buffer):
        part = buffer.at[pl.ds(0, buffer.shape[0] - 1)]
        pltpu.make_async_copy(part, part, recv_sem.at[slot]).wait()

    def sent(slot, buffer):
        part = buffer.at[pl.ds(0, buffer.shape[0] - 1)]
        pltpu.make_async_copy(part, part, send_sem.at[slot]).wait()

    def summed_slots(first, recv):
        def add(k, total):
            return total + recv[k].astype(F32)

        return lax.fori_loop(1, n_grp, add, first.astype(F32))

    barrier = pltpu.get_barrier_semaphore()

    def greet(k, carry):
        pl.semaphore_signal(
            barrier, inc=1, device_id={"grp": lax.rem(me_g + k, n_grp)}, device_id_type=MESH
        )
        return carry

    lax.fori_loop(1, n_grp, greet, 0)
    for k in range(1, n_tp):
        pl.semaphore_signal(
            barrier, inc=1, device_id={"tp": lax.rem(me_t + k, n_tp)}, device_id_type=MESH
        )
    load_state = pltpu.make_async_copy(state_hbm, state_v, load_sem.at[0])
    load_inject = pltpu.make_async_copy(inject_hbm, inject_v, load_sem.at[1])
    load_down = pltpu.make_async_copy(down_hbm, down_v, load_sem.at[2])
    load_state.start()
    load_inject.start()
    load_down.start()

    def up_copy(i):
        rows = pl.ds(pl.multiple_of(i * ROWS, ROWS), ROWS)
        return pltpu.make_async_copy(up_hbm.at[rows], up_v.at[rows], up_sem.at[i])

    chunks = hidden // ROWS
    for i in range(chunks):
        up_copy(i).start()
    pl.semaphore_wait(barrier, n_grp - 1 + n_tp - 1)

    over_tp(0, lambda p: pair_ref, lambda k: pairs_v.at[me_t])
    over_grp(1, lambda p: tall_ref, lambda k: tall_v.at[me_g])
    pairs_v[me_t] = pair_ref[...]
    tall_v[me_g] = tall_ref[...]

    load_state.wait()
    load_inject.wait()
    step_rows = 160

    def add_rows(i, square):
        rows = pl.ds(pl.multiple_of(i * step_rows, step_rows), step_rows)
        value = state_v[rows].astype(F32) + inject_v[rows].astype(F32)
        summed_v[rows] = value
        return square + (value * value).reshape(step_rows // 8, 8, tokens).sum(axis=0)

    square = lax.fori_loop(0, width // step_rows, add_rows, jnp.zeros((8, tokens), F32))
    summed_v[pl.ds(width, 16)] = jnp.zeros((16, tokens), F32)
    square = square.sum(axis=0, keepdims=True)
    mean1 = square / width + epsilon
    rho1 = lax.rsqrt(mean1)
    norm1 = jnp.sqrt(mean1)

    def scale_rows(i, carry):
        rows = pl.ds(pl.multiple_of(i * step_rows, step_rows), step_rows)
        normed_v[rows] = (summed_v[rows] * rho1).astype(BF16)
        return carry

    lax.fori_loop(0, width // step_rows, scale_rows, 0)

    def block_rows(i, carry):
        for part in range(8):
            base = pl.multiple_of(i * (8 * cols) + part * cols // 8 * 8, 8)
            value = summed_v[pl.ds(base, tall + 8)]
            shift = part * cols % 8
            blocks_v[i * 8 + part] = (value[shift : shift + tall] * rho1).astype(BF16)
        return carry

    lax.fori_loop(0, n_grp // 8, block_rows, 0)

    arrived(0, pairs_v)
    load_down.wait()
    up_cols = pairs_v[:, :own].reshape(units, cols)
    down_cols = pairs_v[:, own:].reshape(units, cols)
    own_down = pair_ref[own:]
    spans = [(c, min(640, hidden - c)) for c in range(0, hidden, 640)]
    for c, w in spans:
        m_send[:, :, c : c + w] = dot(down_cols, down_v[:, c : c + w]).reshape(n_grp, 8, w).astype(BF16)
    if wide > hidden:
        m_send[:, :, hidden:wide] = jnp.zeros((n_grp, 8, wide - hidden), BF16)
    grams = jnp.concatenate([dot(own_down, down_cols, NT), dot(own_down, up_cols, NT)], axis=0)
    half = n_grp // 2
    m_send[:half, :, wide:] = grams[:, :TILE].reshape(half, 8, TILE).astype(BF16)
    m_send[half:, :, wide:] = grams[:, TILE:].reshape(half, 8, TILE).astype(BF16)
    over_grp(2, lambda p: m_send.at[p], lambda k: m_recv.at[k])

    def up_rows(i, carry):
        up_copy(i).wait()
        rows = pl.ds(pl.multiple_of(i * ROWS, ROWS), ROWS)
        hidden_v[rows] = jax.nn.silu(dot(up_v[rows], normed_v[...])).astype(BF16)
        return carry

    lax.fori_loop(0, chunks, up_rows, 0)

    arrived(1, tall_v)
    group = 4

    def logit_rows(j, total):
        a = tall_v[pl.ds(j * group, group)].reshape(group * tall, 2 * own)
        b = blocks_v[pl.ds(j * group, group)].reshape(group * tall, tokens)
        return total + dot(a, b, TN)

    z_all[me_t] = lax.fori_loop(0, n_grp // group, logit_rows, jnp.zeros((2 * own, tokens), F32))
    over_tp(3, lambda p: z_all.at[me_t], lambda k: z_all.at[me_t])

    arrived(2, m_recv)
    m_full[me_g] = summed_slots(m_send[me_g], m_recv).astype(BF16)
    over_grp(4, lambda p: m_full.at[me_g], lambda k: m_full.at[me_g])
    arrived(4, m_full)

    low = m_full[:half, :, wide:].reshape(2 * own, TILE)
    high = m_full[half:, :, wide:].reshape(2 * own, TILE)
    small_all[me_t] = jnp.concatenate([low, high], axis=1)
    over_tp(5, lambda p: small_all.at[me_t], lambda k: small_all.at[me_t])
    teach = m_full[:, :, :hidden].reshape(units, hidden)
    term = dot(teach, hidden_v[...])
    term_own[...] = term.astype(BF16)
    over_tp(6, lambda p: term_own, lambda k: term_all.at[k])

    arrived(3, z_all)
    arrived(5, small_all)
    gram = small_all[:, :own].reshape(units, units)
    cross = small_all[:, own:].reshape(units, units)
    logits1 = z_all[:, :own].reshape(units, tokens)
    along = z_all[:, own:].reshape(units, tokens) * norm1
    upward = logits1 * norm1
    taught = flag_ref[0:1]
    deep = flag_ref[1:2]
    hidden1 = jax.nn.silu(logits1).astype(BF16)
    gram1 = dot(gram, hidden1)
    hidden1_f = hidden1.astype(F32)
    moved = along + gram1
    square2 = square + jnp.sum(hidden1_f * (along + moved), axis=0, keepdims=True)
    rho2 = lax.rsqrt(jnp.maximum(square2, 0.0) / width + epsilon)
    upward2 = upward + dot(cross, hidden1, TN)
    logits2 = upward2 * rho2
    hidden2 = (jax.nn.silu(logits2) * deep).astype(BF16)
    total_f = hidden1_f + hidden2.astype(F32)
    total = total_f.astype(BF16)
    taught_total = (total_f * taught).astype(BF16)
    for c, w in spans:
        part = dot(taught_total, hidden_v[c : c + w], NT) * (-scale)
        g_send[:, :, c : c + w] = part.reshape(n_grp, 8, w).astype(BF16)
    over_grp(7, lambda p: g_send.at[p], lambda k: g_recv.at[k])

    arrived(6, term_all)
    for k in range(1, n_tp):
        term = term + term_all[k].astype(F32)
    slope = scale * (gram1 + dot(gram, hidden2) - term * taught)
    q2 = slope * silu_slope(logits2) * deep
    mu = jnp.sum(upward2 * q2, axis=0, keepdims=True) / width
    rq2 = (rho2 * q2).astype(BF16)
    ratio = rho2 * rho2 * rho2 * mu
    slope1 = slope + dot(cross, rq2) - ratio * moved
    q1 = slope1 * silu_slope(logits1)
    rq2_f = rq2.astype(F32)
    keep[0] = q1 + rq2_f * norm1
    keep[1] = -hidden1_f * (ratio * norm1)
    keep[2] = total_f
    keep[3] = hidden1_f * ratio
    keep[4] = hidden1_f
    keep[5] = rq2_f
    mine = pl.ds(pl.multiple_of(me_t * own, own), own)
    left = jnp.concatenate([keep[0, mine], keep[1, mine]], axis=0).astype(BF16)

    def direct_rows(j, carry):
        b = blocks_v[pl.ds(j * group, group)].reshape(group * tall, tokens)
        f_send[pl.ds(j * group, group)] = dot(b, left, NT).reshape(group, tall, 2 * own).astype(BF16)
        return carry

    lax.fori_loop(0, n_grp // group, direct_rows, 0)
    c1 = scale * dot(keep[2, mine].astype(BF16), total, NT) - dot(keep[3, mine].astype(BF16), hidden1, NT)
    c2 = dot(keep[4, mine].astype(BF16), rq2, NT)
    c3 = dot(keep[5, mine].astype(BF16), hidden1, NT)
    folded = jnp.concatenate([c1, c2, c3, jnp.zeros((own, units), F32)], axis=0)
    c_send[...] = folded.reshape(n_grp, 8, units).astype(BF16)
    over_grp(8, lambda p: c_send.at[p], lambda k: c_recv.at[k])
    over_grp(9, lambda p: f_send.at[p], lambda k: f_recv.at[k])

    arrived(7, g_recv)
    g_full[me_g] = summed_slots(g_send[me_g], g_recv).astype(BF16)
    over_grp(10, lambda p: g_full.at[me_g], lambda k: g_full.at[me_g])
    arrived(8, c_recv)
    c_full[me_g] = summed_slots(c_send[me_g], c_recv).astype(BF16)
    over_grp(11, lambda p: c_full.at[me_g], lambda k: c_full.at[me_g])
    arrived(9, f_recv)
    direct_ref[...] = summed_slots(f_send[me_g], f_recv)
    arrived(10, g_full)
    out_send[...] = dot(g_full[...].reshape(units, hidden), down_v[...], NT).reshape(n_tp, own, cols)
    over_tp(12, lambda p: out_send.at[p], lambda k: out_recv.at[k])
    arrived(11, c_full)
    folded = c_full[...].reshape(units, units)
    up_cols = pairs_v[:, :own].reshape(units, cols)
    down_cols = pairs_v[:, own:].reshape(units, cols)
    down_rest = dot(folded[:own], down_cols) + dot(folded[own : 2 * own], up_cols)
    rest_ref[:own] = dot(folded[2 * own : 3 * own], down_cols)
    arrived(12, out_recv)
    down_rest = down_rest + out_send[me_t]
    for k in range(1, n_tp):
        down_rest = down_rest + out_recv[k]
    rest_ref[own:] = down_rest

    sent(0, pairs_v)
    sent(1, tall_v)
    sent(2, m_recv)
    sent(3, z_all)
    sent(4, m_full)
    sent(5, small_all)
    sent(6, term_all)
    sent(7, g_recv)
    sent(8, c_recv)
    sent(9, f_recv)
    sent(10, g_full)
    sent(11, c_full)
    sent(12, out_recv)


def body(
    teacher_state,
    injection,
    teacher_up,
    teacher_down,
    student_up,
    student_down,
    teacher_step,
    student_depth,
):
    n_tp, n_grp = lax.axis_size("tp"), lax.axis_size("grp")
    tokens, width = teacher_state.shape
    cols, own = student_up.shape
    units = own * n_tp
    hidden = teacher_down.shape[0]
    scale = loss_scale * 2.0 / (tokens * n_grp)
    tall = ceil_to(cols, 16)
    wide = ceil_to(hidden, TILE)

    pair = jnp.concatenate([student_up.T, student_down], axis=0)
    tall_pair = jnp.pad(pair.T, ((0, tall - cols), (0, 0)))
    sequence = lax.axis_index("grp") * tokens // LENGTH
    here = jnp.arange(teacher_step.shape[0], dtype=jnp.int32) == sequence
    taught = jnp.sum(jnp.where(here & (teacher_step == 1), 1.0, 0.0))
    deep = jnp.sum(jnp.where(here & (student_depth == 2), 1.0, 0.0))
    flags = jnp.where(jnp.arange(8)[:, None] == 0, taught, deep) + jnp.zeros((8, tokens), F32)

    any_spec = pl.BlockSpec(memory_space=pl.ANY)
    vmem = pl.BlockSpec(memory_space=pltpu.VMEM)
    chunk = (n_grp, 8, hidden)
    direct, rest = pl.pallas_call(
        functools.partial(kernel, n_tp, n_grp, (tokens, width, cols, own, hidden, wide, scale)),
        out_shape=(
            jax.ShapeDtypeStruct((tall, 2 * own), F32),
            jax.ShapeDtypeStruct((2 * own, cols), F32),
        ),
        in_specs=[any_spec] * 4 + [vmem] * 3,
        out_specs=(vmem, vmem),
        scratch_shapes=[
            pltpu.VMEM((width, tokens), BF16),
            pltpu.VMEM((width, tokens), BF16),
            pltpu.VMEM((hidden, width), BF16),
            pltpu.VMEM((cols, hidden), BF16),
            pltpu.VMEM((width + 16, tokens), F32),
            pltpu.VMEM((width, tokens), BF16),
            pltpu.VMEM((n_grp, tall, tokens), BF16),
            pltpu.VMEM((hidden, tokens), BF16),
            pltpu.VMEM((n_tp, 2 * own, cols), BF16),
            pltpu.VMEM((n_grp, tall, 2 * own), BF16),
            pltpu.VMEM((n_grp, 8, wide + TILE), BF16),
            pltpu.VMEM((n_grp, 8, wide + TILE), BF16),
            pltpu.VMEM((n_grp, 8, wide + TILE), BF16),
            pltpu.VMEM(chunk, BF16),
            pltpu.VMEM(chunk, BF16),
            pltpu.VMEM(chunk, BF16),
            pltpu.VMEM((n_grp, 8, units), BF16),
            pltpu.VMEM((n_grp, 8, units), BF16),
            pltpu.VMEM((n_grp, 8, units), BF16),
            pltpu.VMEM((n_grp, tall, 2 * own), BF16),
            pltpu.VMEM((n_grp, tall, 2 * own), BF16),
            pltpu.VMEM((n_tp, 2 * own, tokens), F32),
            pltpu.VMEM((n_tp, 2 * own, units), BF16),
            pltpu.VMEM((n_tp, units, tokens), BF16),
            pltpu.VMEM((units, tokens), BF16),
            pltpu.VMEM((n_tp, own, cols), F32),
            pltpu.VMEM((n_tp, own, cols), F32),
            pltpu.VMEM((6, units, tokens), F32),
            pltpu.SemaphoreType.DMA((3,)),
            pltpu.SemaphoreType.DMA((hidden // ROWS,)),
            pltpu.SemaphoreType.DMA((13,)),
            pltpu.SemaphoreType.DMA((13,)),
        ],
        compiler_params=pltpu.CompilerParams(
            collective_id=0, has_side_effects=True, vmem_limit_bytes=67043328
        ),
    )(teacher_state.T, injection.T, teacher_up.T, teacher_down.T, tall_pair, pair, flags)
    grad_up = direct[:cols, :own] + rest[:own].T
    grad_down = direct[:cols, own:].T + rest[own:]
    return (grad_up, grad_down)


def solution(mesh):
    in_specs = (
        P("grp", None),
        P("grp", None),
        P(None, "tp"),
        P("tp", "grp"),
        P("grp", "tp"),
        P("tp", "grp"),
        P(),
        P(),
    )
    out_specs = (P("grp", "tp"), P("tp", "grp"))
    return jax.shard_map(body, mesh=mesh, in_specs=in_specs, out_specs=out_specs, check_vma=False)
```

```python
import functools

import jax
import jax.numpy as jnp
from jax import lax
from jax.experimental import pallas as pl
from jax.experimental.pallas import tpu as pltpu
from jax.sharding import PartitionSpec as P

LENGTH = 1024
epsilon = 1e-06
loss_scale = 64.0
F32 = jnp.float32
BF16 = jnp.bfloat16
MESH = pl.DeviceIdType.MESH
NN = ((1,), (0,))
NT = ((1,), (1,))
TN = ((0,), (0,))
ROWS = 320
TILE = 128
GRID = (4, 4, 2)
GATHER_ORDERS = ((1, 2, 0), (2, 0, 1), (0, 1, 2))


def lane_cuts(*ends):
    starts = (0, *ends[:-1])
    return tuple((slice(None), pl.ds(a * TILE, (b - a) * TILE)) for a, b in zip(starts, ends))


def row_cuts(*ends):
    starts = (0, *ends[:-1])
    return tuple((pl.ds(a * 8, (b - a) * 8), slice(None)) for a, b in zip(starts, ends))


M_CUTS = lane_cuts(6, 12, 18)
F_CUTS = row_cuts(7, 14, 22)


def room_shapes(rows, lanes, cuts):
    rooms = []
    for order, (r, c) in zip(GATHER_ORDERS, cuts):
        tail = (rows if r == slice(None) else r.size, lanes if c == slice(None) else c.size)
        sizes = [GRID[a] for a in order]
        middle = tuple(GRID[a] for a in sorted(order[:2]))
        landing = (
            pltpu.VMEM((sizes[2] - 1, *middle, *tail), BF16),
            pltpu.VMEM((sizes[1] - 1, sizes[0], *tail), BF16),
            pltpu.VMEM((sizes[0] - 1, *tail), BF16),
        )
        held = (pltpu.VMEM((*middle, *tail), BF16), pltpu.VMEM((sizes[0], *tail), BF16))
        rooms.append((landing, held))
    return rooms


def dot(a, b, dims=NN):
    return lax.dot_general(a, b, (dims, ((), ())), preferred_element_type=F32)


def silu_slope(logits):
    sigmoid = jax.nn.sigmoid(logits)
    return sigmoid * (1.0 + logits * (1.0 - sigmoid))


def ceil_to(value, multiple):
    return -(-value // multiple) * multiple


def kernel(
    n_tp,
    n_grp,
    sizes,
    state_hbm,
    inject_hbm,
    up_hbm,
    down_hbm,
    tall_ref,
    pair_ref,
    step_ref,
    depth_ref,
    direct_ref,
    rest_ref,
    state_v,
    inject_v,
    up_v,
    down_v,
    summed_v,
    normed_v,
    blocks_v,
    hidden_v,
    pairs_v,
    tall_v,
    m_send,
    m_full,
    g_send,
    g_full,
    c_send,
    c_recv,
    c_full,
    k_send,
    k_recv,
    k_full,
    f_send,
    stages,
    z_all,
    small_all,
    term_f32,
    term_send,
    term_recv,
    half_send,
    half_recv,
    term_sum,
    out_part,
    out_pair,
    out_send,
    out_last,
    keep,
    load_sem,
    up_sem,
    send_sem,
    recv_sem,
    stage_send,
    stage_recv,
    tp_send,
    tp_recv,
):
    tokens, width, cols, own, hidden, wide, scale = sizes
    units = own * n_tp
    tall = tall_ref.shape[0]
    me_g = lax.axis_index("grp")
    me_t = lax.axis_index("tp")
    me = (me_g // (GRID[1] * GRID[2]), me_g // GRID[2] % GRID[1], me_g % GRID[2])

    def along_axis(axis, coord):
        z, x, y = (coord if a == axis else me[a] for a in range(3))
        return {"grp": (z * GRID[1] + x) * GRID[2] + y}

    def remote(source, target, slot, device):
        pltpu.make_async_remote_copy(
            src_ref=source,
            dst_ref=target,
            send_sem=stage_send.at[slot],
            recv_sem=stage_recv.at[slot],
            device_id=device,
            device_id_type=MESH,
        ).start()

    pending = []

    def wait_bytes(part, sem):
        pltpu.make_async_copy(part, part, sem).wait()

    def gather_start(slot, buffer, cuts, stage):
        for p, order in enumerate(GATHER_ORDERS):
            axis = order[stage]
            where = [me[a] for a in range(3)]
            for a in order[:stage]:
                where[a] = pl.ds(0, GRID[a])
            part = buffer.at[(*where, *cuts[p])]
            for k in range(1, GRID[axis]):
                peer = lax.rem(me[axis] + k, GRID[axis])
                remote(part, part, slot + 3 * p + stage, along_axis(axis, peer))
            where[axis] = pl.ds(0, GRID[axis] - 1)
            pending.append((buffer.at[(*where, *cuts[p])], stage_send.at[slot + 3 * p + stage]))

    def gather_wait(slot, buffer, cuts, stage):
        for p, order in enumerate(GATHER_ORDERS):
            axis = order[stage]
            where = [me[a] for a in range(3)]
            for a in order[:stage]:
                where[a] = pl.ds(0, GRID[a])
            where[axis] = pl.ds(0, GRID[axis] - 1)
            wait_bytes(buffer.at[(*where, *cuts[p])], stage_recv.at[slot + 3 * p + stage])

    def scatter_start(slot, buffer, rooms, cuts, stage):
        for p, order in enumerate(GATHER_ORDERS):
            axis = order[2 - stage]
            landing, held = rooms[p]
            for k in range(1, GRID[axis]):
                peer = lax.rem(me[axis] + k, GRID[axis])
                if stage == 0:
                    where = [pl.ds(0, GRID[a]) for a in range(3)]
                    where[axis] = peer
                    source = buffer.at[(*where, *cuts[p])]
                elif stage == 1:
                    source = held[0].at[peer] if axis < order[0] else held[0].at[:, peer]
                else:
                    source = held[1].at[peer]
                remote(source, landing[stage].at[k - 1], slot + 3 * p + stage, along_axis(axis, peer))
            pending.append((landing[stage], stage_send.at[slot + 3 * p + stage]))

    def scatter_sum(slot, buffer, rooms, cuts, stage, finish=None):
        for p, order in enumerate(GATHER_ORDERS):
            axis = order[2 - stage]
            landing, held = rooms[p]
            wait_bytes(landing[stage], stage_recv.at[slot + 3 * p + stage])
            if stage == 0:
                where = [slice(None)] * 3
                where[axis] = me[axis]
                mine = buffer[(*where, *cuts[p])]
            elif stage == 1:
                mine = held[0][me[axis]] if axis < order[0] else held[0][:, me[axis]]
            else:
                mine = held[1][me[axis]]
            value = mine.astype(F32)
            for k in range(GRID[axis] - 1):
                value = value + landing[stage][k].astype(F32)
            if stage == 2:
                finish(cuts[p], value)
            else:
                held[stage][...] = value.astype(BF16)

    def over_grp(slot, source, target):
        def step(k, carry):
            peer = lax.rem(me_g + k, n_grp)
            pltpu.make_async_remote_copy(
                src_ref=source(peer),
                dst_ref=target(k),
                send_sem=send_sem.at[slot],
                recv_sem=recv_sem.at[slot],
                device_id={"grp": peer},
                device_id_type=MESH,
            ).start()
            return carry

        lax.fori_loop(1, n_grp, step, 0)

    mate = me_t + 1 - 2 * (me_t % 2)
    across = lax.rem(me_t + n_tp // 2, n_tp)

    def to_tp(slot, source, target, peer):
        pltpu.make_async_remote_copy(
            src_ref=source,
            dst_ref=target,
            send_sem=tp_send.at[slot],
            recv_sem=tp_recv.at[slot],
            device_id={"tp": peer},
            device_id_type=MESH,
        ).start()
        pending.append((source, tp_send.at[slot]))

    def tp_first(slot, source, buffer):
        to_tp(slot, source, buffer.at[me_t], across)
        to_tp(slot + 1, source, buffer.at[me_t], mate)

    def tp_second(slot, buffer):
        wait_bytes(buffer.at[across], tp_recv.at[slot])
        to_tp(slot + 2, buffer.at[across], buffer.at[across], mate)

    def tp_last(slot, buffer):
        wait_bytes(buffer.at[0], tp_recv.at[slot + 1])
        wait_bytes(buffer.at[0], tp_recv.at[slot + 2])

    def arrived(slot, buffer):
        part = buffer.at[pl.ds(0, buffer.shape[0] - 1)]
        pltpu.make_async_copy(part, part, recv_sem.at[slot]).wait()

    def sent(slot, buffer):
        part = buffer.at[pl.ds(0, buffer.shape[0] - 1)]
        pltpu.make_async_copy(part, part, send_sem.at[slot]).wait()

    def summed_slots(first, recv):
        def add(k, total):
            return total + recv[k].astype(F32)

        return lax.fori_loop(1, n_grp, add, first.astype(F32))

    barrier = pltpu.get_barrier_semaphore()

    def greet(k, carry):
        pl.semaphore_signal(
            barrier, inc=1, device_id={"grp": lax.rem(me_g + k, n_grp)}, device_id_type=MESH
        )
        return carry

    lax.fori_loop(1, n_grp, greet, 0)
    for k in range(1, n_tp):
        pl.semaphore_signal(
            barrier, inc=1, device_id={"tp": lax.rem(me_t + k, n_tp)}, device_id_type=MESH
        )
    load_state = pltpu.make_async_copy(state_hbm, state_v, load_sem.at[0])
    load_inject = pltpu.make_async_copy(inject_hbm, inject_v, load_sem.at[1])
    load_down = pltpu.make_async_copy(down_hbm, down_v, load_sem.at[2])
    tall_load = pltpu.make_async_copy(tall_ref, tall_v.at[me], load_sem.at[3])
    tall_load.start()
    load_state.start()
    load_inject.start()
    load_down.start()

    def up_copy(i):
        rows = pl.ds(pl.multiple_of(i * ROWS, ROWS), ROWS)
        return pltpu.make_async_copy(up_hbm.at[rows], up_v.at[rows], up_sem.at[i])

    chunks = hidden // ROWS
    pl.semaphore_wait(barrier, n_grp - 1 + n_tp - 1)

    tp_first(0, pair_ref, pairs_v)
    pairs_v[me_t] = pair_ref[...]
    tall_load.wait()
    gather_start(0, tall_v, F_CUTS, 0)
    m_rooms, g_rooms, f_rooms = stages

    load_state.wait()
    load_inject.wait()
    for i in range(chunks):
        up_copy(i).start()
    step_rows = 160

    def add_rows(i, square):
        rows = pl.ds(pl.multiple_of(i * step_rows, step_rows), step_rows)
        value = state_v[rows].astype(F32) + inject_v[rows].astype(F32)
        summed_v[rows] = value
        return square + (value * value).reshape(step_rows // 8, 8, tokens).sum(axis=0)

    square = lax.fori_loop(0, width // step_rows, add_rows, jnp.zeros((8, tokens), F32))
    summed_v[pl.ds(width, 16)] = jnp.zeros((16, tokens), F32)
    square = square.sum(axis=0, keepdims=True)
    mean1 = square / width + epsilon
    rho1 = lax.rsqrt(mean1)
    norm1 = jnp.sqrt(mean1)

    tp_second(0, pairs_v)
    gather_wait(0, tall_v, F_CUTS, 0)
    gather_start(0, tall_v, F_CUTS, 1)

    def scale_rows(i, carry):
        rows = pl.ds(pl.multiple_of(i * step_rows, step_rows), step_rows)
        normed_v[rows] = (summed_v[rows] * rho1).astype(BF16)
        return carry

    lax.fori_loop(0, width // step_rows, scale_rows, 0)

    tp_last(0, pairs_v)
    up_cols = pairs_v[:, :own].reshape(units, cols)
    down_cols = pairs_v[:, own:].reshape(units, cols)
    own_down = pair_ref[own:]
    grams = jnp.concatenate([dot(own_down, down_cols, NT), dot(own_down, up_cols, NT)], axis=0)
    half = n_grp // 2
    k_send[:half] = grams[:, :TILE].reshape(half, 8, TILE)
    k_send[half:] = grams[:, TILE:].reshape(half, 8, TILE)
    over_grp(1, lambda p: k_send.at[p], lambda k: k_recv.at[k])
    load_down.wait()
    spans = [(c, min(640, hidden - c)) for c in range(0, hidden, 640)]
    for c, w in spans:
        part = dot(down_cols, down_v[:, c : c + w])
        m_send[:, :, :, :, c : c + w] = part.reshape(*GRID, 8, w).astype(BF16)
    blank = jnp.zeros((*GRID, 8, wide - hidden), BF16)
    m_send[:, :, :, :, hidden:wide] = blank
    gather_wait(0, tall_v, F_CUTS, 1)
    gather_start(0, tall_v, F_CUTS, 2)
    scatter_start(9, m_send, m_rooms, M_CUTS, 0)

    def block_rows(i, carry):
        for part in range(8):
            base = pl.multiple_of(i * (8 * cols) + part * cols // 8 * 8, 8)
            value = summed_v[pl.ds(base, tall + 8)]
            shift = part * cols % 8
            blocks_v[i * 8 + part] = (value[shift : shift + tall] * rho1).astype(BF16)
        return carry

    lax.fori_loop(0, n_grp // 8, block_rows, 0)

    def up_rows(i, carry):
        up_copy(i).wait()
        rows = pl.ds(pl.multiple_of(i * ROWS, ROWS), ROWS)
        hidden_v[rows] = jax.nn.silu(dot(up_v[rows], normed_v[...])).astype(BF16)
        return carry

    lax.fori_loop(0, 2, up_rows, 0)
    arrived(1, k_recv)
    k_full[me_g] = summed_slots(k_send[me_g], k_recv)
    over_grp(2, lambda p: k_full.at[me_g], lambda k: k_full.at[me_g])
    scatter_sum(9, m_send, m_rooms, M_CUTS, 0)
    scatter_start(9, m_send, m_rooms, M_CUTS, 1)
    lax.fori_loop(2, 5, up_rows, 0)
    scatter_sum(9, m_send, m_rooms, M_CUTS, 1)
    scatter_start(9, m_send, m_rooms, M_CUTS, 2)
    lax.fori_loop(5, chunks, up_rows, 0)

    def into(buffer):
        def finish(cut, value):
            buffer[(*me, *cut)] = value.astype(BF16)

        return finish

    gather_wait(0, tall_v, F_CUTS, 2)
    group = GRID[1] * GRID[2]

    def logit_rows(j, total):
        a = tall_v[j].reshape(group * tall, 2 * own)
        b = blocks_v[pl.ds(j * group, group)].reshape(group * tall, tokens)
        return total + dot(a, b, TN)

    z_all[me_t] = lax.fori_loop(0, GRID[0], logit_rows, jnp.zeros((2 * own, tokens), F32))
    tp_first(3, z_all.at[me_t], z_all)
    scatter_sum(9, m_send, m_rooms, M_CUTS, 2, into(m_full))
    gather_start(18, m_full, M_CUTS, 0)
    arrived(2, k_full)
    low = k_full[:half].reshape(2 * own, TILE)
    high = k_full[half:].reshape(2 * own, TILE)
    small_all[me_t] = jnp.concatenate([low, high], axis=1)
    tp_first(6, small_all.at[me_t], small_all)
    tp_second(3, z_all)
    tp_second(6, small_all)
    gather_wait(18, m_full, M_CUTS, 0)
    gather_start(18, m_full, M_CUTS, 1)

    tp_last(3, z_all)
    tp_last(6, small_all)
    gram_f = small_all[:, :own].reshape(units, units)
    gram_hi = gram_f.astype(BF16)
    gram_lo = (gram_f - gram_hi.astype(F32)).astype(BF16)
    cross = small_all[:, own:].reshape(units, units).astype(BF16)

    def gram_dot(value):
        return dot(gram_hi, value) + dot(gram_lo, value)

    logits1 = z_all[:, :own].reshape(units, tokens)
    along = z_all[:, own:].reshape(units, tokens) * norm1
    upward = logits1 * norm1
    sequence = me_g * tokens // LENGTH
    taught = jnp.where(step_ref[sequence] == 1, 1.0, 0.0)
    deep = jnp.where(depth_ref[sequence] == 2, 1.0, 0.0)
    hidden1 = jax.nn.silu(logits1).astype(BF16)
    gram1 = gram_dot(hidden1)
    hidden1_f = hidden1.astype(F32)
    moved = along + gram1
    square2 = square + jnp.sum(hidden1_f * (along + moved), axis=0, keepdims=True)
    rho2 = lax.rsqrt(jnp.maximum(square2, 0.0) / width + epsilon)
    upward2 = upward + dot(cross, hidden1, TN)
    logits2 = upward2 * rho2
    hidden2 = (jax.nn.silu(logits2) * deep).astype(BF16)
    total_f = hidden1_f + hidden2.astype(F32)
    total = total_f.astype(BF16)
    taught_total = (total_f * taught).astype(BF16)
    for c, w in spans:
        part = dot(taught_total, hidden_v[c : c + w], NT) * (-scale)
        g_send[:, :, :, :, c : c + w] = part.reshape(*GRID, 8, w).astype(BF16)
    g_send[:, :, :, :, hidden:wide] = blank
    scatter_start(27, g_send, g_rooms, M_CUTS, 0)

    gather_wait(18, m_full, M_CUTS, 1)
    gather_start(18, m_full, M_CUTS, 2)
    scatter_sum(27, g_send, g_rooms, M_CUTS, 0)
    scatter_start(27, g_send, g_rooms, M_CUTS, 1)
    gather_wait(18, m_full, M_CUTS, 2)

    teach = m_full[:, :, :, :, :hidden].reshape(units, hidden)
    term = dot(teach, hidden_v[...])
    term_send[...] = term.astype(BF16)
    to_tp(9, term_send, term_recv, mate)
    core = me_t % 2
    core_rows = pl.ds(pl.multiple_of(core * TILE, TILE), TILE)
    wait_bytes(term_recv, tp_recv.at[9])
    term_f32[...] = term + term_recv[...].astype(F32)
    half_send[...] = term_f32[core_rows].astype(BF16)
    to_tp(10, half_send, half_recv, across)
    scatter_sum(27, g_send, g_rooms, M_CUTS, 1)
    scatter_start(27, g_send, g_rooms, M_CUTS, 2)
    wait_bytes(half_recv, tp_recv.at[10])
    term_sum[core] = term_f32[core_rows] + half_recv[...].astype(F32)
    to_tp(11, term_sum.at[core], term_sum.at[core], mate)
    scatter_sum(27, g_send, g_rooms, M_CUTS, 2, into(g_full))
    gather_start(45, g_full, M_CUTS, 0)
    wait_bytes(term_sum.at[0], tp_recv.at[11])
    term = term_sum[...].reshape(units, tokens)

    slope = scale * (gram1 + gram_dot(hidden2) - term * taught)
    q2 = slope * silu_slope(logits2) * deep
    mu = jnp.sum(upward2 * q2, axis=0, keepdims=True) / width
    rq2 = (rho2 * q2).astype(BF16)
    ratio = rho2 * rho2 * rho2 * mu
    slope1 = slope + dot(cross, rq2) - ratio * moved
    q1 = slope1 * silu_slope(logits1)
    rq2_f = rq2.astype(F32)
    keep[0] = q1 + rq2_f * norm1
    keep[1] = -hidden1_f * (ratio * norm1)
    keep[2] = total_f
    keep[3] = hidden1_f * ratio
    keep[4] = hidden1_f
    keep[5] = rq2_f
    mine = pl.ds(pl.multiple_of(me_t * own, own), own)
    left = jnp.concatenate([keep[0, mine], keep[1, mine]], axis=0).astype(BF16)

    def direct_rows(j, carry):
        b = blocks_v[pl.ds(j * group, group)].reshape(group * tall, tokens)
        f_send[j] = dot(b, left, NT).reshape(*GRID[1:], tall, 2 * own).astype(BF16)
        return carry

    lax.fori_loop(0, GRID[0], direct_rows, 0)
    c1 = scale * dot(keep[2, mine].astype(BF16), total, NT) - dot(keep[3, mine].astype(BF16), hidden1, NT)
    c2 = dot(keep[4, mine].astype(BF16), rq2, NT)
    c3 = dot(keep[5, mine].astype(BF16), hidden1, NT)
    folded = jnp.concatenate([c1, c2, c3, jnp.zeros((own, units), F32)], axis=0)
    c_send[...] = folded.reshape(n_grp, 8, units).astype(BF16)
    over_grp(8, lambda p: c_send.at[p], lambda k: c_recv.at[k])
    scatter_start(36, f_send, f_rooms, F_CUTS, 0)
    gather_wait(45, g_full, M_CUTS, 0)
    gather_start(45, g_full, M_CUTS, 1)
    arrived(8, c_recv)
    c_full[me_g] = summed_slots(c_send[me_g], c_recv).astype(BF16)
    over_grp(11, lambda p: c_full.at[me_g], lambda k: c_full.at[me_g])
    gather_wait(45, g_full, M_CUTS, 1)
    gather_start(45, g_full, M_CUTS, 2)
    scatter_sum(36, f_send, f_rooms, F_CUTS, 0)
    scatter_start(36, f_send, f_rooms, F_CUTS, 1)

    def to_direct(cut, value):
        direct_ref[cut] = value

    scatter_sum(36, f_send, f_rooms, F_CUTS, 1)
    scatter_start(36, f_send, f_rooms, F_CUTS, 2)
    gather_wait(45, g_full, M_CUTS, 2)
    outer = g_full[:, :, :, :, :hidden].reshape(units, hidden)
    out_part[...] = dot(outer, down_v[...], NT).reshape(2, 2, own, cols)
    to_tp(12, out_part.at[:, 1 - core], out_pair, mate)
    scatter_sum(36, f_send, f_rooms, F_CUTS, 2, to_direct)
    wait_bytes(out_pair, tp_recv.at[12])
    out_send[...] = out_part[across // 2, core] + out_pair[across // 2]
    to_tp(13, out_send, out_last, across)
    arrived(11, c_full)
    folded = c_full[...].reshape(units, units)
    up_cols = pairs_v[:, :own].reshape(units, cols)
    down_cols = pairs_v[:, own:].reshape(units, cols)
    down_rest = dot(folded[:own], down_cols) + dot(folded[own : 2 * own], up_cols)
    rest_ref[:own] = dot(folded[2 * own : 3 * own], down_cols)
    down_rest = down_rest + out_part[me_t // 2, core] + out_pair[me_t // 2]
    wait_bytes(out_last, tp_recv.at[13])
    rest_ref[own:] = down_rest + out_last[...]

    sent(1, k_recv)
    sent(2, k_full)
    sent(8, c_recv)
    sent(11, c_full)
    for part, sem in pending:
        wait_bytes(part, sem)


def body(
    teacher_state,
    injection,
    teacher_up,
    teacher_down,
    student_up,
    student_down,
    teacher_step,
    student_depth,
):
    n_tp, n_grp = lax.axis_size("tp"), lax.axis_size("grp")
    tokens, width = teacher_state.shape
    cols, own = student_up.shape
    units = own * n_tp
    hidden = teacher_down.shape[0]
    scale = loss_scale * 2.0 / (tokens * n_grp)
    tall = ceil_to(cols, 16)
    wide = ceil_to(hidden, TILE)

    pair = jnp.concatenate([student_up.T, student_down], axis=0)
    tall_pair = jnp.pad(pair.T, ((0, tall - cols), (0, 0)))
    any_spec = pl.BlockSpec(memory_space=pl.ANY)
    vmem = pl.BlockSpec(memory_space=pltpu.VMEM)
    smem = pl.BlockSpec(memory_space=pltpu.SMEM)
    chunk = (*GRID, 8, wide)
    direct, rest = pl.pallas_call(
        functools.partial(kernel, n_tp, n_grp, (tokens, width, cols, own, hidden, wide, scale)),
        out_shape=(
            jax.ShapeDtypeStruct((tall, 2 * own), F32),
            jax.ShapeDtypeStruct((2 * own, cols), F32),
        ),
        in_specs=[any_spec] * 4 + [vmem] * 2 + [smem] * 2,
        out_specs=(vmem, vmem),
        scratch_shapes=[
            pltpu.VMEM((width, tokens), BF16),
            pltpu.VMEM((width, tokens), BF16),
            pltpu.VMEM((hidden, width), BF16),
            pltpu.VMEM((cols, hidden), BF16),
            pltpu.VMEM((width + 16, tokens), F32),
            pltpu.VMEM((width, tokens), BF16),
            pltpu.VMEM((n_grp, tall, tokens), BF16),
            pltpu.VMEM((hidden, tokens), BF16),
            pltpu.VMEM((n_tp, 2 * own, cols), BF16),
            pltpu.VMEM((*GRID, tall, 2 * own), BF16),
            pltpu.VMEM(chunk, BF16),
            pltpu.VMEM(chunk, BF16),
            pltpu.VMEM(chunk, BF16),
            pltpu.VMEM(chunk, BF16),
            pltpu.VMEM((n_grp, 8, units), BF16),
            pltpu.VMEM((n_grp, 8, units), BF16),
            pltpu.VMEM((n_grp, 8, units), BF16),
            pltpu.VMEM((n_grp, 8, TILE), F32),
            pltpu.VMEM((n_grp, 8, TILE), F32),
            pltpu.VMEM((n_grp, 8, TILE), F32),
            pltpu.VMEM((*GRID, tall, 2 * own), BF16),
            (
                room_shapes(8, wide, M_CUTS),
                room_shapes(8, wide, M_CUTS),
                room_shapes(tall, 2 * own, F_CUTS),
            ),
            pltpu.VMEM((n_tp, 2 * own, tokens), F32),
            pltpu.VMEM((n_tp, 2 * own, units), F32),
            pltpu.VMEM((units, tokens), F32),
            pltpu.VMEM((units, tokens), BF16),
            pltpu.VMEM((units, tokens), BF16),
            pltpu.VMEM((units // 2, tokens), BF16),
            pltpu.VMEM((units // 2, tokens), BF16),
            pltpu.VMEM((2, units // 2, tokens), F32),
            pltpu.VMEM((2, 2, own, cols), F32),
            pltpu.VMEM((2, own, cols), F32),
            pltpu.VMEM((own, cols), F32),
            pltpu.VMEM((own, cols), F32),
            pltpu.VMEM((6, units, tokens), F32),
            pltpu.SemaphoreType.DMA((4,)),
            pltpu.SemaphoreType.DMA((hidden // ROWS,)),
            pltpu.SemaphoreType.DMA((13,)),
            pltpu.SemaphoreType.DMA((13,)),
            pltpu.SemaphoreType.DMA((54,)),
            pltpu.SemaphoreType.DMA((54,)),
            pltpu.SemaphoreType.DMA((14,)),
            pltpu.SemaphoreType.DMA((14,)),
        ],
        compiler_params=pltpu.CompilerParams(
            collective_id=0, has_side_effects=True, vmem_limit_bytes=67043328
        ),
    )(teacher_state.T, injection.T, teacher_up.T, teacher_down.T, tall_pair, pair, teacher_step, student_depth)
    grad_up = direct[:cols, :own] + rest[:own].T
    grad_down = direct[:cols, own:].T + rest[own:]
    return (grad_up, grad_down)


def solution(mesh):
    in_specs = (
        P("grp", None),
        P("grp", None),
        P(None, "tp"),
        P("tp", "grp"),
        P("grp", "tp"),
        P("tp", "grp"),
        P(),
        P(),
    )
    out_specs = (P("grp", "tp"), P("tp", "grp"))
    return jax.shard_map(body, mesh=mesh, in_specs=in_specs, out_specs=out_specs, check_vma=False)
```
